256 devices in a mesh: intv: 1, node: 16 (over y, x), row: 16 (over z, core).
Axes of the slice: x: 4, y: 4, z: 8, core: 2. Of those that a mesh axis runs over, the one named last changes fastest.
Arguments:
- inv_factors: float32 [16, 16, 2, 512, 512], P(('intv', 'node'), 'row'), may hold values from -0.48535534 to 0.48535534, as said below
- coupling: float32 [16, 512, 512], P('row'), may hold values from -0.5 to 0.5
- vectors: float32 [16, 512, 64], P('row'), may hold values from -6 to 6
Outputs:
- moments: float32 [16, 512, 256], P(('intv', 'row'), 'node')
- gram: float32 [256, 256], P('intv')
The draws below stay inside these ranges and needn't reach their ends.
Inputs may be any that keep to these rules, and one draw needn't show every extreme that they name: `inv_factors`: each [j, k] entry holds the real part then the imaginary part of a full 512 x 512 inverse factor.
All inputs are finite; a program needn't handle non-finite values.
Results may differ from the reference program's by a relative error of at most 0.0003.
Values sent between devices are 32-bit elements; how exact they have to be, the bound alone decides.
A program may use at most 64 MiB of HBM per device.

```python
import functools
import math
import jax
import jax.numpy as jnp
from jax import lax

BS = 512
NVEC = 64
MOM = 2
NB = 16
NQ = 16
NROWS = 8192
COLS = 256


def draw_inv_factors(key, part):
    key_off, key_mag, key_phase = jax.random.split(jax.random.fold_in(key, 17), 3)
    spread = 0.2 / math.sqrt(BS)
    offdiag = jax.random.truncated_normal(key_off, -4.0, 4.0, (NQ, NB, 2, BS, BS), jnp.float32) * spread
    magnitude = jax.random.uniform(key_mag, (NQ, NB, 1, BS), jnp.float32, 0.2, 0.45)
    phase = jax.random.uniform(key_phase, (NQ, NB, 1, BS), jnp.float32, -math.pi, math.pi)
    diagonal = jnp.concatenate([magnitude * jnp.cos(phase), magnitude * jnp.sin(phase)], axis=2)
    identity = jnp.eye(BS, dtype=jnp.float32)
    return offdiag + diagonal[..., None] * identity


def block_scale(stream_key, shape, cuts, low, top_value):
    loudness = 1.0
    for position, blocks in cuts:
        steps = jax.random.uniform(jax.random.fold_in(jax.random.fold_in(stream_key, 6), position), (blocks,), jnp.float32, low / len(cuts), top_value / len(cuts))
        loudness = loudness * jnp.repeat(jnp.exp(steps), shape[position] // blocks).reshape((-1,) + (1,) * (len(shape) - 1 - position))
    return loudness


def normal_values(own_key, shape, scale, limit, cuts=(), held_as=jnp.bfloat16):
    level = block_scale(own_key, shape, cuts, -0.22, 0.18) if cuts else 1.0
    entries = jax.random.normal(own_key, shape, jnp.float32) * scale * level
    return jnp.minimum(jnp.maximum(entries, -limit), limit).astype(held_as)


def setup_inputs(seed: int = 0, part: int = 0) -> dict:
    streams_of = jax.random.split(jax.random.key(seed), 4)
    part_keys = jax.random.split(jax.random.fold_in(streams_of[3], part), 4)
    inv_factors = draw_inv_factors(jax.random.fold_in(jax.random.fold_in(streams_of[3], part), 71), part)
    coupling = normal_values(streams_of[1], (NB, BS, BS), (BS // 4) ** -0.5, 0.5, ((0, 16),), jnp.float32)
    vectors = normal_values(streams_of[2], (NB, BS, NVEC), 1.0, 6.0, ((0, 16),), jnp.float32)
    return {"inv_factors": inv_factors, "coupling": coupling, "vectors": vectors}


HIGH = lax.Precision.HIGHEST


def complex_product(factor, block):
    half = block.shape[1] // 2
    real_side = jnp.dot(factor[0], block, precision=HIGH)
    imag_side = jnp.dot(factor[1], block, precision=HIGH)
    return jnp.concatenate([real_side[:, :half] - imag_side[:, half:], real_side[:, half:] + imag_side[:, :half]], axis=1)


def solve_node(factors, coupling, vectors):
    filler = jnp.zeros((BS, NVEC), jnp.float32)
    carry = jnp.zeros((BS, 2 * NVEC), jnp.float32)
    forward = []
    for block_id in range(NB):
        start = jnp.concatenate([vectors[block_id], filler], axis=1) + carry
        upper = complex_product(factors[block_id], start)
        forward.append(upper)
        carry = jnp.dot(coupling[block_id].T, upper, precision=HIGH)
    solved = [None] * NB
    solved[NB - 1] = forward[NB - 1]
    for block_id in range(NB - 2, -1, -1):
        coupled = jnp.dot(coupling[block_id], solved[block_id + 1], precision=HIGH)
        solved[block_id] = forward[block_id] + complex_product(factors[block_id], coupled)
    return jnp.stack(solved)


def reference(inv_factors, coupling, vectors):
    solver = functools.partial(solve_node, coupling=coupling, vectors=vectors)
    solutions = lax.map(solver, inv_factors)
    nodes_index = jnp.arange(NQ).astype(jnp.float32)
    theta = 2.0 * math.pi * (nodes_index + 0.5) / NQ
    real_sol = solutions[..., :NVEC]
    imag_sol = solutions[..., NVEC:]
    pieces = []
    for order in range(MOM):
        w_real = jnp.cos((order + 1) * theta) / NQ
        w_imag = jnp.sin((order + 1) * theta) / NQ
        pieces.append(jnp.einsum('q,qbrc->brc', w_real, real_sol) - jnp.einsum('q,qbrc->brc', w_imag, imag_sol))
        pieces.append(jnp.einsum('q,qbrc->brc', w_real, imag_sol) + jnp.einsum('q,qbrc->brc', w_imag, real_sol))
    moments = jnp.concatenate(pieces, axis=-1)
    flat = moments.reshape(NROWS, COLS)
    gram = jnp.einsum('rc,rd->cd', flat, flat, precision=HIGH) * (NQ / NROWS)
    return moments, gram
```

```python
import math

import jax
import jax.numpy as jnp
from jax import lax
from jax.experimental import pallas as pl
from jax.experimental.pallas import tpu as pltpu
from jax.sharding import PartitionSpec as P

F32 = jnp.float32
BF16 = jnp.bfloat16
MESH = pl.DeviceIdType.MESH

BS = 512
NVEC = 64
NODES = 16
ROWS = 16
SHARE = BS // NODES
COLS = 256
PIECE = COLS // NODES
NCH = 4
HALF = NVEC // NCH
CH = 2 * HALF


def split(x):
    high = x.astype(BF16)
    return high, (x - high.astype(F32)).astype(BF16)


def dot(a, b):
    return jnp.dot(a, b, preferred_element_type=F32)


def dot3(ah, al, bh, bl):
    return dot(ah, bh) + (dot(ah, bl) + dot(al, bh))


def complex_apply(both, wh, wl):
    n = both.shape[0] // 2
    z = dot(both, wh[...])
    z = z[:n] + (z[n:] + dot(both[:n], wl[...]))
    h = n // 2
    return jnp.concatenate([z[:h, :BS] - z[h:, BS:], z[:h, BS:] + z[h:, :BS]], axis=0)


def stacked(x):
    high, low = split(x)
    return jnp.concatenate([high, low], axis=0)


def kernel(inv, coup, vec, mom, gram,
           a_f, c_f, v_f, vt, ath, atl, ch, cl, cth, ctl, mth, mtl, nth, ntl,
           yhl, fr, fs, br, xs, ub, xt, xa, xr, ga, gr, pa, pr, qa, go,
           in_sem, fss, frs, bss, brs, xss, xrs, gss, grs, pss, prs, qss, qrs):
    k = lax.axis_index("row")
    n = lax.axis_index("node")
    last = ROWS - 1

    loads = [
        pltpu.make_async_copy(inv.at[0, 0, 0], a_f.at[0], in_sem.at[0]),
        pltpu.make_async_copy(inv.at[0, 0, 1], a_f.at[1], in_sem.at[1]),
        pltpu.make_async_copy(coup.at[0], c_f, in_sem.at[2]),
        pltpu.make_async_copy(vec.at[0], v_f, in_sem.at[3]),
    ]
    for load in loads:
        load.start()

    barrier = pltpu.get_barrier_semaphore()

    @pl.loop(1, NODES)
    def _(d):
        pl.semaphore_signal(barrier, inc=1, device_id={"node": lax.rem(n + d, NODES)}, device_id_type=MESH)

    @pl.loop(1, ROWS)
    def _(d):
        pl.semaphore_signal(barrier, inc=1, device_id={"row": lax.rem(k + d, ROWS)}, device_id_type=MESH)

    for part in range(2):
        loads[part].wait()
        for b in range(4):
            high, low = split(a_f[part, b * 128:(b + 1) * 128, :].T)
            at = part * BS + b * 128
            ath[:, at:at + 128] = high
            atl[:, at:at + 128] = low
    loads[2].wait()
    for b in range(4):
        rows = slice(b * 128, (b + 1) * 128)
        block = c_f[rows, :]
        high, low = split(block)
        ch[rows, :] = high
        cl[rows, :] = low
        high, low = split(block.T)
        cth[:, rows] = high
        ctl[:, rows] = low

    @pl.loop(0, 4)
    def _(b):
        rows = pl.ds(pl.multiple_of(b * 128, 128), 128)
        for part in range(2):
            cols = slice(part * BS, (part + 1) * BS)
            high, low = split(dot3(ath[rows, cols], atl[rows, cols], ch[...], cl[...]))
            mth[rows, cols] = high
            mtl[rows, cols] = low

    loads[3].wait()
    v_t = v_f[...].T
    for q in range(NCH):
        vt[q] = v_t[q * HALF:(q + 1) * HALF]

    def backward_operator():
        @pl.loop(0, 4)
        def _(b):
            rows = pl.ds(pl.multiple_of(b * 128, 128), 128)
            for part in range(2):
                cols = slice(part * BS, (part + 1) * BS)
                high, low = split(dot3(cth[rows, :], ctl[rows, :], ath[:, cols], atl[:, cols]))
                nth[rows, cols] = high
                ntl[rows, cols] = low

    @pl.when(k >= 2)
    def _():
        backward_operator()

    pl.semaphore_wait(barrier, NODES + ROWS - 2)

    @pl.when(k == 0)
    def _():
        fr[...] = jnp.zeros_like(fr)

    def forward_copy(q):
        return pltpu.make_async_remote_copy(
            src_ref=fs.at[q], dst_ref=fr.at[q], send_sem=fss.at[q], recv_sem=frs.at[q],
            device_id={"row": k + 1}, device_id_type=MESH)

    def backward_copy(q):
        return pltpu.make_async_remote_copy(
            src_ref=xs.at[q], dst_ref=br.at[q], send_sem=bss.at[q], recv_sem=brs.at[q],
            device_id={"row": k - 1}, device_id_type=MESH)

    @pl.loop(0, NCH)
    def _(q):
        @pl.when(k > 0)
        def _():
            forward_copy(q).wait_recv()

        carry = fr[q]
        both = stacked(jnp.concatenate([carry[:HALF] + vt[q], carry[HALF:]], axis=0))
        yhl[q] = both

        @pl.when(k < last)
        def _():
            fs[q] = complex_apply(both, mth, mtl)
            forward_copy(q).start()

        @pl.when(k == last)
        def _():
            xs[q] = complex_apply(both, ath, atl)
            backward_copy(q).start()

    @pl.when(k < 2)
    def _():
        backward_operator()

    @pl.when(k < last)
    def _():
        @pl.loop(0, NCH)
        def _(q):
            ub[q] = complex_apply(yhl[q], ath, atl)

        @pl.loop(0, NCH)
        def _(q):
            backward_copy(q).wait_recv()
            xs[q] = ub[q] + complex_apply(stacked(br[q]), nth, ntl)

            @pl.when(k > 0)
            def _():
                backward_copy(q).start()

    for q in range(NCH):
        x = xs[q]
        xt[q * HALF:(q + 1) * HALF, :] = x[:HALF]
        xt[NVEC + q * HALF:NVEC + (q + 1) * HALF, :] = x[HALF:]
    for b in range(4):
        x = xt[:, b * 128:(b + 1) * 128].T
        for s in range(128 // SHARE):
            xa[b * (128 // SHARE) + s] = x[s * SHARE:(s + 1) * SHARE]
    xr[n] = xa[n]

    def spread(axis, count, me, source, target, send, recv, by_target):
        def copy(d):
            peer = lax.rem(me + d, count)
            return pltpu.make_async_remote_copy(
                src_ref=source.at[peer] if by_target else source, dst_ref=target.at[me],
                send_sem=send.at[d], recv_sem=recv.at[me],
                device_id={axis: peer}, device_id_type=MESH)

        def arrival(d):
            peer = lax.rem(me + d, count)
            return pltpu.make_async_remote_copy(
                src_ref=source.at[peer] if by_target else source, dst_ref=target.at[peer],
                send_sem=send.at[d], recv_sem=recv.at[peer],
                device_id={axis: peer}, device_id_type=MESH)

        @pl.loop(1, count)
        def _(d):
            copy(d).start()

        def finish():
            @pl.loop(1, count)
            def _(d):
                arrival(d).wait_recv()

        def sent():
            @pl.loop(1, count)
            def _(d):
                copy(d).wait_send()

        return finish, sent

    finish, sent_x = spread("node", NODES, n, xa, xr, xss, xrs, True)
    finish()

    parts = []
    lane = lax.broadcasted_iota(jnp.int32, (SHARE, 2 * NVEC), 1)
    for order in (1, 2):
        even = jnp.zeros((SHARE, 2 * NVEC), F32)
        odd = jnp.zeros((SHARE, 2 * NVEC), F32)
        for j in range(NODES):
            theta = 2.0 * math.pi * (j + 0.5) / NODES
            x = xr[j]
            even = even + (math.cos(order * theta) / NODES) * x
            odd = odd + (math.sin(order * theta) / NODES) * x
        odd = pltpu.roll(odd, NVEC, 1)
        parts.append(even + jnp.where(lane < NVEC, -odd, odd))
    f = jnp.concatenate(parts, axis=1)
    mom[...] = f

    fh, fl = split(f)
    th, tl = split(f.T)
    product = dot3(th, tl, fh, fl)
    for j in range(NODES):
        ga[j] = product[j * PIECE:(j + 1) * PIECE]
    gr[n] = ga[n]
    finish, sent_g = spread("node", NODES, n, ga, gr, gss, grs, True)
    finish()
    total = gr[0]
    for j in range(1, NODES):
        total = total + gr[j]
    pa[...] = total
    pr[k] = total
    finish, sent_p = spread("row", ROWS, k, pa, pr, pss, prs, False)
    finish()
    total = pr[0]
    for j in range(1, ROWS):
        total = total + pr[j]
    total = total * (NODES / (ROWS * BS))
    qa[...] = total
    go[n] = total
    finish, sent_q = spread("node", NODES, n, qa, go, qss, qrs, False)
    finish()
    for j in range(NODES):
        gram[j * PIECE:(j + 1) * PIECE, :] = go[j]

    @pl.when(k < last)
    def _():
        @pl.loop(0, NCH)
        def _(q):
            forward_copy(q).wait_send()

    @pl.when(k > 0)
    def _():
        @pl.loop(0, NCH)
        def _(q):
            backward_copy(q).wait_send()

    sent_x()
    sent_g()
    sent_p()
    sent_q()


def shards(inv_factors, coupling, vectors):
    moments, gram = pl.pallas_call(
        kernel,
        out_shape=(
            jax.ShapeDtypeStruct((SHARE, COLS), F32),
            jax.ShapeDtypeStruct((COLS, COLS), F32),
        ),
        in_specs=[pl.BlockSpec(memory_space=pl.ANY)] * 3,
        out_specs=[pl.BlockSpec(memory_space=pltpu.VMEM)] * 2,
        scratch_shapes=[
            pltpu.VMEM((2, BS, BS), F32),
            pltpu.VMEM((BS, BS), F32),
            pltpu.VMEM((BS, NVEC), F32),
            pltpu.VMEM((NCH, HALF, BS), F32),
        ]
        + [pltpu.VMEM((BS, 2 * BS), BF16)] * 2
        + [pltpu.VMEM((BS, BS), BF16)] * 4
        + [pltpu.VMEM((BS, 2 * BS), BF16)] * 4
        + [pltpu.VMEM((NCH, 2 * CH, BS), BF16)]
        + [pltpu.VMEM((NCH, CH, BS), F32)] * 5
        + [
            pltpu.VMEM((2 * NVEC, BS), F32),
            pltpu.VMEM((NODES, SHARE, 2 * NVEC), F32),
            pltpu.VMEM((NODES, SHARE, 2 * NVEC), F32),
            pltpu.VMEM((NODES, PIECE, COLS), F32),
            pltpu.VMEM((NODES, PIECE, COLS), F32),
            pltpu.VMEM((PIECE, COLS), F32),
            pltpu.VMEM((ROWS, PIECE, COLS), F32),
            pltpu.VMEM((PIECE, COLS), F32),
            pltpu.VMEM((NODES, PIECE, COLS), F32),
        ]
        + [pltpu.SemaphoreType.DMA((4,))]
        + [pltpu.SemaphoreType.DMA((NCH,))] * 4
        + [pltpu.SemaphoreType.DMA((16,))] * 8,
        compiler_params=pltpu.CompilerParams(
            collective_id=0, has_side_effects=True, vmem_limit_bytes=56 * 1024 * 1024),
    )(inv_factors, coupling, vectors)
    return moments[None], gram


def solution(mesh):
    return jax.shard_map(
        shards,
        mesh=mesh,
        in_specs=(
            P(("intv", "node"), "row", None, None, None),
            P("row", None, None),
            P("row", None, None),
        ),
        out_specs=(P(("intv", "row"), "node", None), P("intv", None)),
        check_vma=False,
    )
```

```python
import math

import jax
import jax.numpy as jnp
from jax import lax
from jax.experimental import pallas as pl
from jax.experimental.pallas import tpu as pltpu
from jax.sharding import PartitionSpec as P

F32 = jnp.float32
BF16 = jnp.bfloat16
MESH = pl.DeviceIdType.MESH

BS = 512
NVEC = 64
NODES = 16
ROWS = 16
SHARE = BS // NODES
COLS = 256
PIECE = COLS // NODES
NCH = 8
HALF = NVEC // NCH
CH = 2 * HALF


def split(x):
    high = x.astype(BF16)
    return high, (x - high.astype(F32)).astype(BF16)


def dot(a, b):
    return jnp.dot(a, b, preferred_element_type=F32)


def dot3(ah, al, bh, bl):
    return dot(ah, bh) + (dot(ah, bl) + dot(al, bh))


def stacked(x):
    high, low = split(x)
    return jnp.concatenate([high, low], axis=0)


def complex_apply(x, wh, wl, groups=1):
    n = x.shape[0]
    high, low = split(x)
    z = dot(jnp.concatenate([high, low], axis=0), wh[...])
    z = z[:n] + (z[n:] + dot(high, wl[...]))
    h = n // groups // 2
    out = []
    for g in range(groups):
        re = slice(2 * g * h, (2 * g + 1) * h)
        im = slice((2 * g + 1) * h, (2 * g + 2) * h)
        out.append(z[re, :BS] - z[im, BS:])
        out.append(z[re, BS:] + z[im, :BS])
    return jnp.concatenate(out, axis=0)


def apply_all(x, wh, wl):
    return complex_apply(x.reshape(NCH * CH, BS), wh, wl, NCH).reshape(NCH, CH, BS)


def kernel(inv, coup, vec, mom, gram,
           a_f, c_f, v_f, vt, vo, ath, atl, ch, cl, cth, ctl, mth, mtl, nth, ntl, pth, ptl, qth, qtl,
           snd, rcv, qf, yb, dd, fr, cf, fo, fs, us, uo, es, eo, br, xe, xs,
           xt, xa, xr, ga, gr, pa, pr, qa, go,
           in_sem, pss, prs, css, crs, xss, xrs, gss, grs, hss, hrs, qss, qrs):
    k = lax.axis_index("row")
    n = lax.axis_index("node")
    core = lax.rem(k, 2)
    z = lax.div(k, 2)
    top = ROWS // 2 - 1
    partner = k + 1 - 2 * core

    loads = [
        pltpu.make_async_copy(inv.at[0, 0, 0], a_f.at[0], in_sem.at[0]),
        pltpu.make_async_copy(inv.at[0, 0, 1], a_f.at[1], in_sem.at[1]),
        pltpu.make_async_copy(coup.at[0], c_f, in_sem.at[2]),
        pltpu.make_async_copy(vec.at[0], v_f, in_sem.at[3]),
    ]
    for load in loads:
        load.start()

    barrier = pltpu.get_barrier_semaphore()

    @pl.loop(1, NODES)
    def _(d):
        pl.semaphore_signal(barrier, inc=1, device_id={"node": lax.rem(n + d, NODES)}, device_id_type=MESH)

    @pl.loop(1, ROWS)
    def _(d):
        pl.semaphore_signal(barrier, inc=1, device_id={"row": lax.rem(k + d, ROWS)}, device_id_type=MESH)

    for part in range(2):
        loads[part].wait()
        for b in range(4):
            high, low = split(a_f[part, b * 128:(b + 1) * 128, :].T)
            at = part * BS + b * 128
            ath[:, at:at + 128] = high
            atl[:, at:at + 128] = low
    loads[2].wait()
    for b in range(4):
        rows = slice(b * 128, (b + 1) * 128)
        block = c_f[rows, :]
        high, low = split(block)
        ch[rows, :] = high
        cl[rows, :] = low
        high, low = split(block.T)
        cth[:, rows] = high
        ctl[:, rows] = low
    loads[3].wait()
    v_t = v_f[...].T
    for q in range(NCH):
        vt[q] = v_t[q * HALF:(q + 1) * HALF]

    def block_loop(count):
        def wrap(step):
            @pl.loop(0, count)
            def _(b):
                step(pl.ds(pl.multiple_of(b * (BS // count), BS // count), BS // count))
        return wrap

    def forward_operator(keep):
        @block_loop(4)
        def _(rows):
            for part in range(2):
                cols = slice(part * BS, (part + 1) * BS)
                value = dot3(ath[rows, cols], atl[rows, cols], ch[...], cl[...])
                if keep:
                    snd[rows, cols] = value
                high, low = split(value)
                mth[rows, cols] = high
                mtl[rows, cols] = low

    def backward_operator(keep):
        @block_loop(4)
        def _(rows):
            for part in range(2):
                cols = slice(part * BS, (part + 1) * BS)
                value = dot3(cth[rows, :], ctl[rows, :], ath[:, cols], atl[:, cols])
                if keep:
                    snd[rows, cols] = value
                high, low = split(value)
                nth[rows, cols] = high
                ntl[rows, cols] = low

    def compose(left, rows, wh, wl):
        x = jnp.concatenate([left[rows, :BS], left[rows, BS:]], axis=0)
        out = complex_apply(x, wh, wl)
        half = out.shape[0] // 2
        return out[:half], out[half:]

    def store_split(rows, parts, wh, wl):
        for part, value in enumerate(parts):
            cols = slice(part * BS, (part + 1) * BS)
            high, low = split(value)
            wh[rows, cols] = high
            wl[rows, cols] = low

    def chunk_copy(kind, source, target, row):
        def make(q):
            return pltpu.make_async_remote_copy(
                src_ref=source.at[q], dst_ref=target.at[q], send_sem=css.at[kind, q], recv_sem=crs.at[kind, q],
                device_id={"row": row}, device_id_type=MESH)
        return make

    def whole_copy(kind, source, target):
        return pltpu.make_async_remote_copy(
            src_ref=source, dst_ref=target, send_sem=pss.at[kind], recv_sem=prs.at[kind],
            device_id={"row": partner}, device_id_type=MESH)

    forward = chunk_copy(0, fs, fr, k + 2)
    relay = chunk_copy(1, fr, cf, partner)
    inner = chunk_copy(2, fs, fo, partner)
    upper = chunk_copy(3, us, uo, partner)
    term = chunk_copy(4, es, eo, partner)
    backward = chunk_copy(5, xe, br, k - 2)
    solved = chunk_copy(6, xe, xs, partner)
    operator = whole_copy(0, snd, rcv)
    probe = whole_copy(1, vt, vo)
    second = whole_copy(2, qf, qf)

    def chunks(step):
        @pl.loop(0, NCH)
        def _(q):
            step(q)

    def shifted_by(carry, v):
        return jnp.concatenate([carry[:HALF] + v, carry[HALF:]], axis=0)

    def enter():
        pl.semaphore_wait(barrier, NODES + ROWS - 2)

    def real_rows(v):
        return jnp.concatenate([v, jnp.zeros_like(v)], axis=0)

    def even_forward(first):
        @chunks
        def _(q):
            if first:
                y = real_rows(vt[q])
            else:
                relay(q).wait_recv()
                y = shifted_by(cf[q], vt[q])
            yb[q] = y
            fs[q] = complex_apply(y, mth, mtl)
            inner(q).start()

    @pl.when(core == 0)
    def _():
        forward_operator(True)
        enter()
        probe.start()

        @pl.when((z > 0) & (z < top))
        def _():
            operator.start()

        @pl.when(z == 0)
        def _():
            even_forward(True)

        backward_operator(False)
        operator.wait_recv()
        probe.wait_recv()

        @pl.when(z < top)
        def _():
            @block_loop(8)
            def _(rows):
                re, im = compose(rcv, rows, nth, ntl)
                qf[rows, :BS] = re
                qf[rows, BS:] = im

        @pl.when(z == top)
        def _():
            @block_loop(8)
            def _(rows):
                store_split(rows, compose(rcv, rows, nth, ntl), pth, ptl)

            @block_loop(8)
            def _(rows):
                re, im = compose(snd, rows, pth, ptl)
                qf[rows, :BS] = re + (ath[rows, :BS].astype(F32) + atl[rows, :BS].astype(F32))
                qf[rows, BS:] = im + (ath[rows, BS:].astype(F32) + atl[rows, BS:].astype(F32))

        second.start()

        @pl.when(z == top)
        def _():
            @chunks
            def _(q):
                es[q] = complex_apply(real_rows(vo[q]), pth, ptl)
                term(q).start()

        @pl.when(z > 0)
        def _():
            even_forward(False)

        @pl.when(z < top)
        def _():
            us[...] = apply_all(yb[...], ath, atl)

            @chunks
            def _(q):
                upper(q).wait_recv()
                es[q] = us[q] + complex_apply(uo[q], nth, ntl)
                term(q).start()

        @chunks
        def _(q):
            solved(q).wait_recv()

    def odd_upper():
        @chunks
        def _(q):
            inner(q).wait_recv()
            yb[q] = shifted_by(fo[q], vt[q])

        us[...] = apply_all(yb[...], ath, atl)

        @chunks
        def _(q):
            upper(q).start()

    @pl.when(core == 1)
    def _():
        @pl.when(z == 0)
        def _():
            forward_operator(False)
            enter()
            probe.start()

            @chunks
            def _(q):
                inner(q).wait_recv()
                y = shifted_by(fo[q], vt[q])
                yb[q] = y
                fs[q] = complex_apply(y, mth, mtl)
                forward(q).start()

            us[...] = apply_all(yb[...], ath, atl)

            @chunks
            def _(q):
                upper(q).start()

            backward_operator(True)
            operator.start()
            probe.wait_recv()

        @pl.when((z > 0) & (z < top))
        def _():
            backward_operator(True)
            enter()
            operator.start()
            probe.start()
            forward_operator(False)

            @chunks
            def _(q):
                dd[q] = complex_apply(real_rows(vt[q]), mth, mtl)

            operator.wait_recv()

            @block_loop(8)
            def _(rows):
                store_split(rows, compose(rcv, rows, mth, mtl), pth, ptl)

            probe.wait_recv()

            @chunks
            def _(q):
                forward(q).wait_recv()
                relay(q).start()
                fs[q] = dd[q] + complex_apply(shifted_by(fr[q], vo[q]), pth, ptl)
                forward(q).start()

            odd_upper()

        def take_second(wh, wl):
            second.wait_recv()

            @block_loop(8)
            def _(rows):
                store_split(rows, (qf[rows, :BS], qf[rows, BS:]), wh, wl)

        @pl.when(z == top)
        def _():
            @block_loop(8)
            def _(rows):
                snd[rows, :] = ath[rows, :].astype(F32) + atl[rows, :].astype(F32)

            enter()
            operator.start()
            probe.start()
            probe.wait_recv()
            take_second(pth, ptl)

            @chunks
            def _(q):
                forward(q).wait_recv()
                relay(q).start()
                term(q).wait_recv()
                xe[q] = eo[q] + complex_apply(shifted_by(fr[q], vo[q]), pth, ptl)
                backward(q).start()
                solved(q).start()

            @chunks
            def _(q):
                inner(q).wait_recv()
                yb[q] = shifted_by(fo[q], vt[q])

            xs[...] = apply_all(yb[...], ath, atl)

        @pl.when(z < top)
        def _():
            take_second(qth, qtl)

            @chunks
            def _(q):
                term(q).wait_recv()
                backward(q).wait_recv()
                xe[q] = eo[q] + complex_apply(br[q], qth, qtl)

                @pl.when(z > 0)
                def _():
                    backward(q).start()

                solved(q).start()

            xs[...] = us[...] + apply_all(br[...], nth, ntl)

    for q in range(NCH):
        x = xs[q]
        xt[q * HALF:(q + 1) * HALF, :] = x[:HALF]
        xt[NVEC + q * HALF:NVEC + (q + 1) * HALF, :] = x[HALF:]
    for b in range(4):
        x = xt[:, b * 128:(b + 1) * 128].T
        for s in range(128 // SHARE):
            xa[b * (128 // SHARE) + s] = x[s * SHARE:(s + 1) * SHARE]
    xr[n] = xa[n]

    def spread(axis, count, me, source, target, send, recv, by_target):
        def copy(d):
            peer = lax.rem(me + d, count)
            return pltpu.make_async_remote_copy(
                src_ref=source.at[peer] if by_target else source, dst_ref=target.at[me],
                send_sem=send.at[d], recv_sem=recv.at[me],
                device_id={axis: peer}, device_id_type=MESH)

        def arrival(d):
            peer = lax.rem(me + d, count)
            return pltpu.make_async_remote_copy(
                src_ref=source.at[peer] if by_target else source, dst_ref=target.at[peer],
                send_sem=send.at[d], recv_sem=recv.at[peer],
                device_id={axis: peer}, device_id_type=MESH)

        @pl.loop(1, count)
        def _(d):
            copy(d).start()

        def finish():
            @pl.loop(1, count)
            def _(d):
                arrival(d).wait_recv()

        def sent():
            @pl.loop(1, count)
            def _(d):
                copy(d).wait_send()

        return finish, sent

    finish, sent_x = spread("node", NODES, n, xa, xr, xss, xrs, True)
    finish()

    parts = []
    lane = lax.broadcasted_iota(jnp.int32, (SHARE, 2 * NVEC), 1)
    for order in (1, 2):
        even = jnp.zeros((SHARE, 2 * NVEC), F32)
        odd = jnp.zeros((SHARE, 2 * NVEC), F32)
        for j in range(NODES):
            theta = 2.0 * math.pi * (j + 0.5) / NODES
            x = xr[j]
            even = even + (math.cos(order * theta) / NODES) * x
            odd = odd + (math.sin(order * theta) / NODES) * x
        odd = pltpu.roll(odd, NVEC, 1)
        parts.append(even + jnp.where(lane < NVEC, -odd, odd))
    f = jnp.concatenate(parts, axis=1)
    mom[...] = f

    fh, fl = split(f)
    th, tl = split(f.T)
    product = dot3(th, tl, fh, fl)
    for j in range(NODES):
        ga[j] = product[j * PIECE:(j + 1) * PIECE]
    gr[n] = ga[n]
    finish, sent_g = spread("node", NODES, n, ga, gr, gss, grs, True)
    finish()
    total = gr[0]
    for j in range(1, NODES):
        total = total + gr[j]
    pa[...] = total
    pr[k] = total
    finish, sent_p = spread("row", ROWS, k, pa, pr, hss, hrs, False)
    finish()
    total = pr[0]
    for j in range(1, ROWS):
        total = total + pr[j]
    total = total * (NODES / (ROWS * BS))
    qa[...] = total
    go[n] = total
    finish, sent_q = spread("node", NODES, n, qa, go, qss, qrs, False)
    finish()
    for j in range(NODES):
        gram[j * PIECE:(j + 1) * PIECE, :] = go[j]

    probe.wait_send()

    @pl.when((core == 1) | ((z > 0) & (z < top)))
    def _():
        operator.wait_send()

    @pl.when(core == 0)
    def _():
        second.wait_send()

        @chunks
        def _(q):
            inner(q).wait_send()
            term(q).wait_send()

    @pl.when(core == 1)
    def _():
        @chunks
        def _(q):
            solved(q).wait_send()

        @pl.when(z > 0)
        def _():
            @chunks
            def _(q):
                relay(q).wait_send()
                backward(q).wait_send()

        @pl.when(z < top)
        def _():
            @chunks
            def _(q):
                forward(q).wait_send()
                upper(q).wait_send()

    sent_x()
    sent_g()
    sent_p()
    sent_q()


def shards(inv_factors, coupling, vectors):
    chunk = pltpu.VMEM((NCH, CH, BS), F32)
    whole = pltpu.VMEM((BS, 2 * BS), F32)
    whole_part = pltpu.VMEM((BS, 2 * BS), BF16)
    square_part = pltpu.VMEM((BS, BS), BF16)
    moments, gram = pl.pallas_call(
        kernel,
        out_shape=(
            jax.ShapeDtypeStruct((SHARE, COLS), F32),
            jax.ShapeDtypeStruct((COLS, COLS), F32),
        ),
        in_specs=[pl.BlockSpec(memory_space=pl.ANY)] * 3,
        out_specs=[pl.BlockSpec(memory_space=pltpu.VMEM)] * 2,
        scratch_shapes=[
            pltpu.VMEM((2, BS, BS), F32),
            pltpu.VMEM((BS, BS), F32),
            pltpu.VMEM((BS, NVEC), F32),
            pltpu.VMEM((NCH, HALF, BS), F32),
            pltpu.VMEM((NCH, HALF, BS), F32),
        ]
        + [whole_part] * 2
        + [square_part] * 4
        + [whole_part] * 8
        + [whole] * 3
        + [chunk] * 13
        + [
            pltpu.VMEM((2 * NVEC, BS), F32),
            pltpu.VMEM((NODES, SHARE, 2 * NVEC), F32),
            pltpu.VMEM((NODES, SHARE, 2 * NVEC), F32),
            pltpu.VMEM((NODES, PIECE, COLS), F32),
            pltpu.VMEM((NODES, PIECE, COLS), F32),
            pltpu.VMEM((PIECE, COLS), F32),
            pltpu.VMEM((ROWS, PIECE, COLS), F32),
            pltpu.VMEM((PIECE, COLS), F32),
            pltpu.VMEM((NODES, PIECE, COLS), F32),
        ]
        + [pltpu.SemaphoreType.DMA((4,))]
        + [pltpu.SemaphoreType.DMA((3,))] * 2
        + [pltpu.SemaphoreType.DMA((7, NCH))] * 2
        + [pltpu.SemaphoreType.DMA((16,))] * 8,
        compiler_params=pltpu.CompilerParams(
            collective_id=0, has_side_effects=True, vmem_limit_bytes=56 * 1024 * 1024),
    )(inv_factors, coupling, vectors)
    return moments[None], gram


def solution(mesh):
    return jax.shard_map(
        shards,
        mesh=mesh,
        in_specs=(
            P(("intv", "node"), "row", None, None, None),
            P("row", None, None),
            P("row", None, None),
        ),
        out_specs=(P(("intv", "row"), "node", None), P("intv", None)),
        check_vma=False,
    )
```

```python
import math

import jax
import jax.numpy as jnp
from jax import lax
from jax.experimental import pallas as pl
from jax.experimental.pallas import tpu as pltpu
from jax.sharding import PartitionSpec as P

F32 = jnp.float32
BF16 = jnp.bfloat16
MESH = pl.DeviceIdType.MESH

BS = 512
NVEC = 64
NODES = 16
ROWS = 16
SHARE = BS // NODES
COLS = 256
PIECE = COLS // NODES // 2
NCH = 8
PARTS = 4
SIDE = 4
HEIGHT = ROWS // 2
HALF = NVEC // NCH
CH = 2 * HALF


def split(x):
    high = x.astype(BF16)
    return high, (x - high.astype(F32)).astype(BF16)


def dot(a, b):
    return jnp.dot(a, b, preferred_element_type=F32)


def dot3(ah, al, bh, bl):
    return dot(ah, bh) + (dot(ah, bl) + dot(al, bh))


def stacked(x):
    high, low = split(x)
    return jnp.concatenate([high, low], axis=0)


def complex_apply(x, wh, wl, groups=1):
    n = x.shape[0]
    high, low = split(x)
    z = dot(jnp.concatenate([high, low], axis=0), wh[...])
    z = z[:n] + (z[n:] + dot(high, wl[...]))
    h = n // groups // 2
    out = []
    for g in range(groups):
        re = slice(2 * g * h, (2 * g + 1) * h)
        im = slice((2 * g + 1) * h, (2 * g + 2) * h)
        out.append(z[re, :BS] - z[im, BS:])
        out.append(z[re, BS:] + z[im, :BS])
    return jnp.concatenate(out, axis=0)


def apply_all(x, wh, wl):
    return complex_apply(x.reshape(NCH * CH, BS), wh, wl, NCH).reshape(NCH, CH, BS)


def kernel(inv, coup, vec, mom, gram,
           a_f, c_f, vt, vo, ath, atl, ch, cl, cth, ctl, mth, mtl, nth, ntl, pth, ptl, qth, qtl,
           snd, rcv, qf, yb, dd, fr, cf, fo, fs, us, uo, es, eo, br, xe, xs,
           xt, xa, xr, ga, gr, pa, pr, qa, go, fb, fp,
           in_sem, oss, ors, pss, prs, css, crs, xss, xrs, gss, grs, hss, hrs, qss, qrs, plane_sem):
    k = lax.axis_index("row")
    n = lax.axis_index("node")
    core = lax.rem(k, 2)
    z = lax.div(k, 2)
    top = ROWS // 2 - 1
    partner = k + 1 - 2 * core

    loads = [
        pltpu.make_async_copy(inv.at[0, 0, 0], a_f.at[0], in_sem.at[0]),
        pltpu.make_async_copy(inv.at[0, 0, 1], a_f.at[1], in_sem.at[1]),
        pltpu.make_async_copy(coup.at[0], c_f, in_sem.at[2]),
        pltpu.make_async_copy(vec, vt, in_sem.at[3]),
    ]
    for load in loads:
        load.start()

    barrier = pltpu.get_barrier_semaphore()

    def plane_signal(sem):
        across = lax.rem(n, SIDE)
        base = n - across
        for d in range(1, SIDE):
            pl.semaphore_signal(sem, inc=1, device_id={"node": base + lax.rem(across + d, SIDE)}, device_id_type=MESH)
            pl.semaphore_signal(sem, inc=1, device_id={"node": lax.rem(n + d * SIDE, NODES)}, device_id_type=MESH)

    plane_signal(barrier)

    pl.semaphore_signal(barrier, inc=1, device_id={"row": partner}, device_id_type=MESH)

    @pl.when(z > 0)
    def _():
        pl.semaphore_signal(barrier, inc=1, device_id={"row": k - 2}, device_id_type=MESH)

    @pl.when(z < top)
    def _():
        pl.semaphore_signal(barrier, inc=1, device_id={"row": k + 2}, device_id_type=MESH)

    for part in range(2):
        loads[part].wait()
        for b in range(4):
            high, low = split(a_f[part, b * 128:(b + 1) * 128, :].T)
            at = part * BS + b * 128
            ath[:, at:at + 128] = high
            atl[:, at:at + 128] = low
    loads[2].wait()
    for b in range(4):
        rows = slice(b * 128, (b + 1) * 128)
        block = c_f[rows, :]
        high, low = split(block)
        ch[rows, :] = high
        cl[rows, :] = low
        high, low = split(block.T)
        cth[:, rows] = high
        ctl[:, rows] = low
    loads[3].wait()

    def block_loop(count):
        def wrap(step):
            @pl.loop(0, count)
            def _(b):
                step(b, pl.ds(pl.multiple_of(b * (BS // count), BS // count), BS // count))
        return wrap

    def forward_operator(keep):
        @block_loop(4)
        def _(b, rows):
            for part in range(2):
                cols = slice(part * BS, (part + 1) * BS)
                value = dot3(ath[rows, cols], atl[rows, cols], ch[...], cl[...])
                if keep:
                    snd[rows, cols] = value
                high, low = split(value)
                mth[rows, cols] = high
                mtl[rows, cols] = low
            if keep:
                @pl.when((z > 0) & (z < top))
                def _():
                    operator(b).start()

    def backward_operator(keep):
        @block_loop(4)
        def _(b, rows):
            for part in range(2):
                cols = slice(part * BS, (part + 1) * BS)
                value = dot3(cth[rows, :], ctl[rows, :], ath[:, cols], atl[:, cols])
                if keep:
                    snd[rows, cols] = value
                high, low = split(value)
                nth[rows, cols] = high
                ntl[rows, cols] = low
            if keep:
                operator(b).start()

    def compose(left, rows, wh, wl):
        x = jnp.concatenate([left[rows, :BS], left[rows, BS:]], axis=0)
        high, low = split(x)
        y = dot3(high, low, wh[...], wl[...])
        half = y.shape[0] // 2
        return y[:half, :BS] - y[half:, BS:], y[:half, BS:] + y[half:, :BS]

    def store_split(rows, parts, wh, wl):
        for part, value in enumerate(parts):
            cols = slice(part * BS, (part + 1) * BS)
            high, low = split(value)
            wh[rows, cols] = high
            wl[rows, cols] = low

    def chunk_copy(kind, source, target, row):
        def make(q):
            return pltpu.make_async_remote_copy(
                src_ref=source.at[q], dst_ref=target.at[q], send_sem=css.at[kind, q], recv_sem=crs.at[kind, q],
                device_id={"row": row}, device_id_type=MESH)
        return make

    def whole_copy(kind, source, target):
        return pltpu.make_async_remote_copy(
            src_ref=source, dst_ref=target, send_sem=pss.at[kind], recv_sem=prs.at[kind],
            device_id={"row": partner}, device_id_type=MESH)

    forward = chunk_copy(0, fs, fr, k + 2)
    relay = chunk_copy(1, fr, cf, partner)
    inner = chunk_copy(2, fs, fo, partner)
    upper = chunk_copy(3, us, uo, partner)
    term = chunk_copy(4, es, eo, partner)
    backward = chunk_copy(5, xe, br, k - 2)
    solved = chunk_copy(6, xe, xs, partner)

    def operator(b):
        rows = pl.ds(pl.multiple_of(b * (BS // PARTS), BS // PARTS), BS // PARTS)
        return pltpu.make_async_remote_copy(
            src_ref=snd.at[rows, :], dst_ref=rcv.at[rows, :], send_sem=oss.at[b], recv_sem=ors.at[b],
            device_id={"row": partner}, device_id_type=MESH)

    probe = whole_copy(1, vt, vo)
    second = whole_copy(2, qf, qf)

    def chunks(step):
        @pl.loop(0, NCH)
        def _(q):
            step(q)

    def shifted_by(carry, v):
        return jnp.concatenate([carry[:HALF] + v, carry[HALF:]], axis=0)

    def enter():
        ends = (z == 0).astype(jnp.int32) + (z == top).astype(jnp.int32)
        pl.semaphore_wait(barrier, 2 * (SIDE - 1) + 3 - ends)
        plane_signal(plane_sem)

    def real_rows(v):
        return jnp.concatenate([v, jnp.zeros_like(v)], axis=0)

    def even_forward(first):
        @chunks
        def _(q):
            if first:
                y = real_rows(vt[q])
            else:
                relay(q).wait_recv()
                y = shifted_by(cf[q], vt[q])
            yb[q] = y
            fs[q] = complex_apply(y, mth, mtl)
            inner(q).start()

    @pl.when(core == 0)
    def _():
        enter()
        probe.start()
        forward_operator(True)

        @pl.when(z == 0)
        def _():
            even_forward(True)

        backward_operator(False)
        probe.wait_recv()

        @pl.when(z < top)
        def _():
            @block_loop(PARTS)
            def _(b, rows):
                operator(b).wait_recv()
                re, im = compose(rcv, rows, nth, ntl)
                qf[rows, :BS] = re
                qf[rows, BS:] = im

        @pl.when(z == top)
        def _():
            @block_loop(PARTS)
            def _(b, rows):
                operator(b).wait_recv()
                store_split(rows, compose(rcv, rows, nth, ntl), pth, ptl)

            @block_loop(PARTS)
            def _(b, rows):
                re, im = compose(snd, rows, pth, ptl)
                qf[rows, :BS] = re + (ath[rows, :BS].astype(F32) + atl[rows, :BS].astype(F32))
                qf[rows, BS:] = im + (ath[rows, BS:].astype(F32) + atl[rows, BS:].astype(F32))

        second.start()

        @pl.when(z == top)
        def _():
            @chunks
            def _(q):
                es[q] = complex_apply(real_rows(vo[q]), pth, ptl)
                term(q).start()

        @pl.when(z > 0)
        def _():
            even_forward(False)

        @pl.when(z < top)
        def _():
            us[...] = apply_all(yb[...], ath, atl)

            @chunks
            def _(q):
                upper(q).wait_recv()
                es[q] = us[q] + complex_apply(uo[q], nth, ntl)
                term(q).start()

        @chunks
        def _(q):
            solved(q).wait_recv()

    def odd_upper():
        @chunks
        def _(q):
            inner(q).wait_recv()
            yb[q] = shifted_by(fo[q], vt[q])

        us[...] = apply_all(yb[...], ath, atl)

        @chunks
        def _(q):
            upper(q).start()

    @pl.when(core == 1)
    def _():
        @pl.when(z == 0)
        def _():
            enter()
            probe.start()
            forward_operator(False)

            @chunks
            def _(q):
                inner(q).wait_recv()
                y = shifted_by(fo[q], vt[q])
                yb[q] = y
                fs[q] = complex_apply(y, mth, mtl)
                forward(q).start()

            us[...] = apply_all(yb[...], ath, atl)

            @chunks
            def _(q):
                upper(q).start()

            backward_operator(True)
            probe.wait_recv()

        @pl.when((z > 0) & (z < top))
        def _():
            enter()
            probe.start()
            forward_operator(False)

            dd[...] = apply_all(jnp.concatenate([vt[...], jnp.zeros_like(vt)], axis=1), mth, mtl)

            @block_loop(PARTS)
            def _(b, rows):
                operator(b).wait_recv()
                store_split(rows, compose(rcv, rows, mth, mtl), pth, ptl)

            probe.wait_recv()

            @pl.when(z > 1)
            def _():
                backward_operator(True)

            @chunks
            def _(q):
                forward(q).wait_recv()
                relay(q).start()
                fs[q] = dd[q] + complex_apply(shifted_by(fr[q], vo[q]), pth, ptl)
                forward(q).start()

            @pl.when(z == 1)
            def _():
                backward_operator(True)

            odd_upper()

        def take_second(wh, wl):
            second.wait_recv()

            @block_loop(8)
            def _(b, rows):
                store_split(rows, (qf[rows, :BS], qf[rows, BS:]), wh, wl)

        @pl.when(z == top)
        def _():
            enter()
            probe.start()

            @block_loop(PARTS)
            def _(b, rows):
                snd[rows, :] = ath[rows, :].astype(F32) + atl[rows, :].astype(F32)
                operator(b).start()

            probe.wait_recv()
            take_second(pth, ptl)

            @chunks
            def _(q):
                forward(q).wait_recv()
                relay(q).start()
                term(q).wait_recv()
                xe[q] = eo[q] + complex_apply(shifted_by(fr[q], vo[q]), pth, ptl)
                backward(q).start()
                solved(q).start()

            @chunks
            def _(q):
                inner(q).wait_recv()
                yb[q] = shifted_by(fo[q], vt[q])

            xs[...] = apply_all(yb[...], ath, atl)

        @pl.when(z < top)
        def _():
            take_second(qth, qtl)

            @chunks
            def _(q):
                term(q).wait_recv()
                backward(q).wait_recv()
                xe[q] = eo[q] + complex_apply(br[q], qth, qtl)

                @pl.when(z > 0)
                def _():
                    backward(q).start()

                solved(q).start()

            xs[...] = us[...] + apply_all(br[...], nth, ntl)

    pl.semaphore_wait(plane_sem, 2 * (SIDE - 1))

    for q in range(NCH):
        x = xs[q]
        xt[q * HALF:(q + 1) * HALF, :] = x[:HALF]
        xt[NVEC + q * HALF:NVEC + (q + 1) * HALF, :] = x[HALF:]
    for b in range(4):
        x = xt[:, b * 128:(b + 1) * 128].T
        for s in range(128 // SHARE):
            xa[b * (128 // SHARE) + s] = x[s * SHARE:(s + 1) * SHARE]
    xr[n] = xa[n]

    def spread(axis, count, me, source, target, send, recv, by_target):
        def copy(d):
            peer = lax.rem(me + d, count)
            return pltpu.make_async_remote_copy(
                src_ref=source.at[peer] if by_target else source, dst_ref=target.at[me],
                send_sem=send.at[d], recv_sem=recv.at[me],
                device_id={axis: peer}, device_id_type=MESH)

        def arrival(d):
            peer = lax.rem(me + d, count)
            return pltpu.make_async_remote_copy(
                src_ref=source.at[peer] if by_target else source, dst_ref=target.at[peer],
                send_sem=send.at[d], recv_sem=recv.at[peer],
                device_id={axis: peer}, device_id_type=MESH)

        @pl.loop(1, count)
        def _(d):
            copy(d).start()

        def finish():
            @pl.loop(1, count)
            def _(d):
                arrival(d).wait_recv()

        def sent():
            @pl.loop(1, count)
            def _(d):
                copy(d).wait_send()

        return finish, sent

    finish, sent_x = spread("node", NODES, n, xa, xr, xss, xrs, True)
    finish()

    parts = []
    lane = lax.broadcasted_iota(jnp.int32, (SHARE, 2 * NVEC), 1)
    for order in (1, 2):
        even = jnp.zeros((SHARE, 2 * NVEC), F32)
        odd = jnp.zeros((SHARE, 2 * NVEC), F32)
        for j in range(NODES):
            theta = 2.0 * math.pi * (j + 0.5) / NODES
            x = xr[j]
            even = even + (math.cos(order * theta) / NODES) * x
            odd = odd + (math.sin(order * theta) / NODES) * x
        odd = pltpu.roll(odd, NVEC, 1)
        parts.append(even + jnp.where(lane < NVEC, -odd, odd))
    f = jnp.concatenate(parts, axis=1)
    mom[...] = f

    fb[...] = f
    other = whole_copy(3, fb, fp)
    other.start()
    other.wait_recv()
    pair = jnp.concatenate([f, fp[...]], axis=0)
    fh, fl = split(pair)
    th, tl = split(jnp.where(core == 0, pair[:, :COLS // 2], pair[:, COLS // 2:]).T)
    product = dot3(th, tl, fh, fl)
    for j in range(NODES):
        ga[j] = product[j * PIECE:(j + 1) * PIECE]
    gr[n] = ga[n]
    finish, sent_g = spread("node", NODES, n, ga, gr, gss, grs, True)
    finish()
    total = gr[0]
    for j in range(1, NODES):
        total = total + gr[j]
    pa[...] = total
    pr[z] = total

    def column(d):
        level = lax.rem(z + d, HEIGHT)
        return pltpu.make_async_remote_copy(
            src_ref=pa, dst_ref=pr.at[z], send_sem=hss.at[d], recv_sem=hrs.at[z],
            device_id={"row": 2 * level + core}, device_id_type=MESH)

    def column_arrival(d):
        level = lax.rem(z + d, HEIGHT)
        return pltpu.make_async_remote_copy(
            src_ref=pa, dst_ref=pr.at[level], send_sem=hss.at[d], recv_sem=hrs.at[level],
            device_id={"row": 2 * level + core}, device_id_type=MESH)

    @pl.loop(1, HEIGHT)
    def _(d):
        column(d).start()

    @pl.loop(1, HEIGHT)
    def _(d):
        column_arrival(d).wait_recv()

    total = pr[0]
    for j in range(1, HEIGHT):
        total = total + pr[j]
    total = total * (NODES / (ROWS * BS))
    qa[...] = total
    go[core, n] = total

    def result(side, d):
        return pltpu.make_async_remote_copy(
            src_ref=qa, dst_ref=go.at[core, n], send_sem=qss.at[side, d], recv_sem=qrs.at[core, n],
            device_id={"node": lax.rem(n + d, NODES), "row": partner if side else k}, device_id_type=MESH)

    def result_arrival(side, d):
        peer = lax.rem(n + d, NODES)
        source = 1 - core if side else core
        return pltpu.make_async_remote_copy(
            src_ref=qa, dst_ref=go.at[source, peer], send_sem=qss.at[side, d], recv_sem=qrs.at[source, peer],
            device_id={"node": peer, "row": partner if side else k}, device_id_type=MESH)

    def results(step):
        @pl.loop(1, NODES)
        def _(d):
            step(0, d)
            step(1, d)

        step(1, 0)

    results(lambda side, d: result(side, d).start())
    results(lambda side, d: result_arrival(side, d).wait_recv())
    for c in range(2):
        for j in range(NODES):
            at = c * (COLS // 2) + j * PIECE
            gram[at:at + PIECE, :] = go[c, j]

    probe.wait_send()

    @pl.when((core == 1) | ((z > 0) & (z < top)))
    def _():
        @pl.loop(0, PARTS)
        def _(b):
            operator(b).wait_send()

    @pl.when(core == 0)
    def _():
        second.wait_send()

        @chunks
        def _(q):
            inner(q).wait_send()
            term(q).wait_send()

    @pl.when(core == 1)
    def _():
        @chunks
        def _(q):
            solved(q).wait_send()

        @pl.when(z > 0)
        def _():
            @chunks
            def _(q):
                relay(q).wait_send()
                backward(q).wait_send()

        @pl.when(z < top)
        def _():
            @chunks
            def _(q):
                forward(q).wait_send()
                upper(q).wait_send()

    sent_x()
    sent_g()
    other.wait_send()

    @pl.loop(1, HEIGHT)
    def _(d):
        column(d).wait_send()

    results(lambda side, d: result(side, d).wait_send())


def shards(inv_factors, coupling, vectors):
    chunk = pltpu.VMEM((NCH, CH, BS), F32)
    whole = pltpu.VMEM((BS, 2 * BS), F32)
    whole_part = pltpu.VMEM((BS, 2 * BS), BF16)
    square_part = pltpu.VMEM((BS, BS), BF16)
    moments, gram = pl.pallas_call(
        kernel,
        out_shape=(
            jax.ShapeDtypeStruct((SHARE, COLS), F32),
            jax.ShapeDtypeStruct((COLS, COLS), F32),
        ),
        in_specs=[pl.BlockSpec(memory_space=pl.ANY)] * 3,
        out_specs=[pl.BlockSpec(memory_space=pltpu.VMEM)] * 2,
        scratch_shapes=[
            pltpu.VMEM((2, BS, BS), F32),
            pltpu.VMEM((BS, BS), F32),
            pltpu.VMEM((NCH, HALF, BS), F32),
            pltpu.VMEM((NCH, HALF, BS), F32),
        ]
        + [whole_part] * 2
        + [square_part] * 4
        + [whole_part] * 8
        + [whole] * 3
        + [chunk] * 13
        + [
            pltpu.VMEM((2 * NVEC, BS), F32),
            pltpu.VMEM((NODES, SHARE, 2 * NVEC), F32),
            pltpu.VMEM((NODES, SHARE, 2 * NVEC), F32),
            pltpu.VMEM((NODES, PIECE, COLS), F32),
            pltpu.VMEM((NODES, PIECE, COLS), F32),
            pltpu.VMEM((PIECE, COLS), F32),
            pltpu.VMEM((HEIGHT, PIECE, COLS), F32),
            pltpu.VMEM((PIECE, COLS), F32),
            pltpu.VMEM((2, NODES, PIECE, COLS), F32),
            pltpu.VMEM((SHARE, COLS), F32),
            pltpu.VMEM((SHARE, COLS), F32),
        ]
        + [pltpu.SemaphoreType.DMA((4,))]
        + [pltpu.SemaphoreType.DMA((PARTS,))] * 2
        + [pltpu.SemaphoreType.DMA((4,))] * 2
        + [pltpu.SemaphoreType.DMA((7, NCH))] * 2
        + [pltpu.SemaphoreType.DMA((16,))] * 6
        + [pltpu.SemaphoreType.DMA((2, 16))] * 2
        + [pltpu.SemaphoreType.REGULAR],
        compiler_params=pltpu.CompilerParams(
            collective_id=0, has_side_effects=True, vmem_limit_bytes=56 * 1024 * 1024),
    )(inv_factors, coupling, jnp.swapaxes(vectors, 1, 2).reshape(NCH, HALF, BS))
    return moments[None], gram


def solution(mesh):
    return jax.shard_map(
        shards,
        mesh=mesh,
        in_specs=(
            P(("intv", "node"), "row", None, None, None),
            P("row", None, None),
            P("row", None, None),
        ),
        out_specs=(P(("intv", "row"), "node", None), P("intv", None)),
        check_vma=False,
    )
```

```python
import math

import jax
import jax.numpy as jnp
from jax import lax
from jax.experimental import pallas as pl
from jax.experimental.pallas import tpu as pltpu
from jax.sharding import PartitionSpec as P

F32 = jnp.float32
BF16 = jnp.bfloat16
MESH = pl.DeviceIdType.MESH

BS = 512
NVEC = 64
NODES = 16
ROWS = 16
SHARE = BS // NODES
COLS = 256
PIECE = COLS // NODES // 2
NCH = 8
PARTS = 4
SIDE = 4
HEIGHT = ROWS // 2
HALF = NVEC // NCH
CH = 2 * HALF


def split(x):
    high = x.astype(BF16)
    return high, (x - high.astype(F32)).astype(BF16)


def dot(a, b):
    return jnp.dot(a, b, preferred_element_type=F32)


def dot3(ah, al, bh, bl):
    return dot(ah, bh) + (dot(ah, bl) + dot(al, bh))


def stacked(x):
    high, low = split(x)
    return jnp.concatenate([high, low], axis=0)


def complex_apply(x, wh, wl, groups=1):
    n = x.shape[0]
    high, low = split(x)
    z = dot(jnp.concatenate([high, low], axis=0), wh[...])
    z = z[:n] + (z[n:] + dot(high, wl[...]))
    h = n // groups // 2
    out = []
    for g in range(groups):
        re = slice(2 * g * h, (2 * g + 1) * h)
        im = slice((2 * g + 1) * h, (2 * g + 2) * h)
        out.append(z[re, :BS] - z[im, BS:])
        out.append(z[re, BS:] + z[im, :BS])
    return jnp.concatenate(out, axis=0)


def apply_all(x, wh, wl):
    return complex_apply(x.reshape(NCH * CH, BS), wh, wl, NCH).reshape(NCH, CH, BS)


def kernel(inv, coup, vt, mom, gram,
           vo, ath, atl, ch, cl, cth, ctl, mth, mtl, nth, ntl, pth, ptl, qth, qtl,
           snd, rcv, qf, yb, dd, fr, cf, fo, fs, us, uo, es, eo, br, xe, xs,
           xt, xa, xr, ga, gr, pa, pr, qa, go, fb, fp,
           oss, ors, pss, prs, css, crs, xss, xrs, gss, grs, hss, hrs, qss, qrs, plane_sem):
    k = lax.axis_index("row")
    n = lax.axis_index("node")
    core = lax.rem(k, 2)
    z = lax.div(k, 2)
    top = ROWS // 2 - 1
    partner = k + 1 - 2 * core

    barrier = pltpu.get_barrier_semaphore()

    def plane_signal(sem):
        across = lax.rem(n, SIDE)
        base = n - across
        for d in range(1, SIDE):
            pl.semaphore_signal(sem, inc=1, device_id={"node": base + lax.rem(across + d, SIDE)}, device_id_type=MESH)
            pl.semaphore_signal(sem, inc=1, device_id={"node": lax.rem(n + d * SIDE, NODES)}, device_id_type=MESH)

    plane_signal(barrier)

    pl.semaphore_signal(barrier, inc=1, device_id={"row": partner}, device_id_type=MESH)

    @pl.when(z > 0)
    def _():
        pl.semaphore_signal(barrier, inc=1, device_id={"row": k - 2}, device_id_type=MESH)

    @pl.when(z < top)
    def _():
        pl.semaphore_signal(barrier, inc=1, device_id={"row": k + 2}, device_id_type=MESH)

    for part in range(2):
        for b in range(4):
            high, low = split(inv[0, 0, part, b * 128:(b + 1) * 128, :].T)
            at = part * BS + b * 128
            ath[:, at:at + 128] = high
            atl[:, at:at + 128] = low
    for b in range(4):
        rows = slice(b * 128, (b + 1) * 128)
        block = coup[0, rows, :]
        high, low = split(block)
        ch[rows, :] = high
        cl[rows, :] = low
        high, low = split(block.T)
        cth[:, rows] = high
        ctl[:, rows] = low

    def block_loop(count):
        def wrap(step):
            @pl.loop(0, count)
            def _(b):
                step(b, pl.ds(pl.multiple_of(b * (BS // count), BS // count), BS // count))
        return wrap

    def forward_operator(keep):
        @block_loop(4)
        def _(b, rows):
            for part in range(2):
                cols = slice(part * BS, (part + 1) * BS)
                value = dot3(ath[rows, cols], atl[rows, cols], ch[...], cl[...])
                if keep:
                    snd[rows, cols] = value
                high, low = split(value)
                mth[rows, cols] = high
                mtl[rows, cols] = low
            if keep:
                @pl.when(b == 0)
                def _():
                    enter()
                    probe.start()

                @pl.when((z > 0) & (z < top))
                def _():
                    operator(b).start()

    def backward_operator(keep):
        @block_loop(4)
        def _(b, rows):
            for part in range(2):
                cols = slice(part * BS, (part + 1) * BS)
                value = dot3(cth[rows, :], ctl[rows, :], ath[:, cols], atl[:, cols])
                if keep:
                    snd[rows, cols] = value
                high, low = split(value)
                nth[rows, cols] = high
                ntl[rows, cols] = low
            if keep:
                operator(b).start()

    def compose(left, rows, wh, wl):
        x = jnp.concatenate([left[rows, :BS], left[rows, BS:]], axis=0)
        high, low = split(x)
        y = dot3(high, low, wh[...], wl[...])
        half = y.shape[0] // 2
        return y[:half, :BS] - y[half:, BS:], y[:half, BS:] + y[half:, :BS]

    def store_split(rows, parts, wh, wl):
        for part, value in enumerate(parts):
            cols = slice(part * BS, (part + 1) * BS)
            high, low = split(value)
            wh[rows, cols] = high
            wl[rows, cols] = low

    def chunk_copy(kind, source, target, row):
        def make(q):
            return pltpu.make_async_remote_copy(
                src_ref=source.at[q], dst_ref=target.at[q], send_sem=css.at[kind, q], recv_sem=crs.at[kind, q],
                device_id={"row": row}, device_id_type=MESH)
        return make

    def whole_copy(kind, source, target):
        return pltpu.make_async_remote_copy(
            src_ref=source, dst_ref=target, send_sem=pss.at[kind], recv_sem=prs.at[kind],
            device_id={"row": partner}, device_id_type=MESH)

    forward = chunk_copy(0, fs, fr, k + 2)
    relay = chunk_copy(1, fr, cf, partner)
    inner = chunk_copy(2, fs, fo, partner)
    upper = chunk_copy(3, us, uo, partner)
    term = chunk_copy(4, es, eo, partner)
    backward = chunk_copy(5, xe, br, k - 2)
    solved = chunk_copy(6, xe, xs, partner)

    def operator(b):
        rows = pl.ds(pl.multiple_of(b * (BS // PARTS), BS // PARTS), BS // PARTS)
        return pltpu.make_async_remote_copy(
            src_ref=snd.at[rows, :], dst_ref=rcv.at[rows, :], send_sem=oss.at[b], recv_sem=ors.at[b],
            device_id={"row": partner}, device_id_type=MESH)

    probe = whole_copy(1, vt, vo)
    second = whole_copy(2, qf, qf)

    def chunks(step):
        @pl.loop(0, NCH)
        def _(q):
            step(q)

    def shifted_by(carry, v):
        return jnp.concatenate([carry[:HALF] + v, carry[HALF:]], axis=0)

    def enter():
        ends = (z == 0).astype(jnp.int32) + (z == top).astype(jnp.int32)
        pl.semaphore_wait(barrier, 2 * (SIDE - 1) + 3 - ends)
        plane_signal(plane_sem)

    def real_rows(v):
        return jnp.concatenate([v, jnp.zeros_like(v)], axis=0)

    def even_forward(first):
        @chunks
        def _(q):
            if first:
                y = real_rows(vt[q])
            else:
                relay(q).wait_recv()
                y = shifted_by(cf[q], vt[q])
            yb[q] = y
            fs[q] = complex_apply(y, mth, mtl)
            inner(q).start()

    @pl.when(core == 0)
    def _():
        forward_operator(True)

        @pl.when(z == 0)
        def _():
            even_forward(True)

        backward_operator(False)
        probe.wait_recv()

        @pl.when(z < top)
        def _():
            @block_loop(PARTS)
            def _(b, rows):
                operator(b).wait_recv()
                re, im = compose(rcv, rows, nth, ntl)
                qf[rows, :BS] = re
                qf[rows, BS:] = im

        @pl.when(z == top)
        def _():
            @block_loop(PARTS)
            def _(b, rows):
                operator(b).wait_recv()
                store_split(rows, compose(rcv, rows, nth, ntl), pth, ptl)

            @block_loop(PARTS)
            def _(b, rows):
                re, im = compose(snd, rows, pth, ptl)
                qf[rows, :BS] = re + (ath[rows, :BS].astype(F32) + atl[rows, :BS].astype(F32))
                qf[rows, BS:] = im + (ath[rows, BS:].astype(F32) + atl[rows, BS:].astype(F32))

        second.start()

        @pl.when(z == top)
        def _():
            @chunks
            def _(q):
                es[q] = complex_apply(real_rows(vo[q]), pth, ptl)
                term(q).start()

        @pl.when(z > 0)
        def _():
            even_forward(False)

        @pl.when(z < top)
        def _():
            us[...] = apply_all(yb[...], ath, atl)

            @chunks
            def _(q):
                upper(q).wait_recv()
                es[q] = us[q] + complex_apply(uo[q], nth, ntl)
                term(q).start()

        @chunks
        def _(q):
            solved(q).wait_recv()

    def odd_upper():
        @chunks
        def _(q):
            inner(q).wait_recv()
            us[q] = complex_apply(shifted_by(fo[q], vt[q]), ath, atl)
            upper(q).start()

    @pl.when(core == 1)
    def _():
        @pl.when(z == 0)
        def _():
            forward_operator(False)
            enter()
            probe.start()

            @chunks
            def _(q):
                inner(q).wait_recv()
                y = shifted_by(fo[q], vt[q])
                yb[q] = y
                fs[q] = complex_apply(y, mth, mtl)
                forward(q).start()

            us[...] = apply_all(yb[...], ath, atl)

            @chunks
            def _(q):
                upper(q).start()

            backward_operator(True)
            probe.wait_recv()

        @pl.when((z > 0) & (z < top))
        def _():
            forward_operator(False)
            enter()
            probe.start()
            dd[...] = apply_all(jnp.concatenate([vt[...], jnp.zeros_like(vt)], axis=1), mth, mtl)

            @block_loop(PARTS)
            def _(b, rows):
                operator(b).wait_recv()
                store_split(rows, compose(rcv, rows, mth, mtl), pth, ptl)

            probe.wait_recv()

            @pl.when(z > 1)
            def _():
                backward_operator(True)

            @chunks
            def _(q):
                forward(q).wait_recv()
                relay(q).start()
                fs[q] = dd[q] + complex_apply(shifted_by(fr[q], vo[q]), pth, ptl)
                forward(q).start()

            @pl.when(z == 1)
            def _():
                backward_operator(True)

            odd_upper()

        def take_second(wh, wl):
            second.wait_recv()

            @block_loop(8)
            def _(b, rows):
                store_split(rows, (qf[rows, :BS], qf[rows, BS:]), wh, wl)

        @pl.when(z == top)
        def _():
            enter()
            probe.start()

            @block_loop(PARTS)
            def _(b, rows):
                snd[rows, :] = ath[rows, :].astype(F32) + atl[rows, :].astype(F32)
                operator(b).start()

            probe.wait_recv()
            take_second(pth, ptl)

            @chunks
            def _(q):
                forward(q).wait_recv()
                relay(q).start()
                term(q).wait_recv()
                xe[q] = eo[q] + complex_apply(shifted_by(fr[q], vo[q]), pth, ptl)
                backward(q).start()
                solved(q).start()

            @chunks
            def _(q):
                inner(q).wait_recv()
                yb[q] = shifted_by(fo[q], vt[q])

            xs[...] = apply_all(yb[...], ath, atl)

        @pl.when(z < top)
        def _():
            take_second(qth, qtl)

            @chunks
            def _(q):
                term(q).wait_recv()
                backward(q).wait_recv()
                xe[q] = eo[q] + complex_apply(br[q], qth, qtl)

                @pl.when(z > 0)
                def _():
                    backward(q).start()

                solved(q).start()

            xs[...] = us[...] + apply_all(br[...], nth, ntl)

    pl.semaphore_wait(plane_sem, 2 * (SIDE - 1))

    for q in range(NCH):
        x = xs[q]
        xt[q * HALF:(q + 1) * HALF, :] = x[:HALF]
        xt[NVEC + q * HALF:NVEC + (q + 1) * HALF, :] = x[HALF:]
    for b in range(4):
        x = xt[:, b * 128:(b + 1) * 128].T
        for s in range(128 // SHARE):
            xa[b * (128 // SHARE) + s] = x[s * SHARE:(s + 1) * SHARE]
    xr[n] = xa[n]

    def spread(axis, count, me, source, target, send, recv, by_target):
        def copy(d):
            peer = lax.rem(me + d, count)
            return pltpu.make_async_remote_copy(
                src_ref=source.at[peer] if by_target else source, dst_ref=target.at[me],
                send_sem=send.at[d], recv_sem=recv.at[me],
                device_id={axis: peer}, device_id_type=MESH)

        def arrival(d):
            peer = lax.rem(me + d, count)
            return pltpu.make_async_remote_copy(
                src_ref=source.at[peer] if by_target else source, dst_ref=target.at[peer],
                send_sem=send.at[d], recv_sem=recv.at[peer],
                device_id={axis: peer}, device_id_type=MESH)

        @pl.loop(1, count)
        def _(d):
            copy(d).start()

        def finish():
            @pl.loop(1, count)
            def _(d):
                arrival(d).wait_recv()

        def sent():
            @pl.loop(1, count)
            def _(d):
                copy(d).wait_send()

        return finish, sent

    finish, sent_x = spread("node", NODES, n, xa, xr, xss, xrs, True)
    finish()

    parts = []
    lane = lax.broadcasted_iota(jnp.int32, (SHARE, 2 * NVEC), 1)
    for order in (1, 2):
        even = jnp.zeros((SHARE, 2 * NVEC), F32)
        odd = jnp.zeros((SHARE, 2 * NVEC), F32)
        for j in range(NODES):
            theta = 2.0 * math.pi * (j + 0.5) / NODES
            x = xr[j]
            even = even + (math.cos(order * theta) / NODES) * x
            odd = odd + (math.sin(order * theta) / NODES) * x
        odd = pltpu.roll(odd, NVEC, 1)
        parts.append(even + jnp.where(lane < NVEC, -odd, odd))
    f = jnp.concatenate(parts, axis=1)
    mom[...] = f

    fb[...] = f
    other = whole_copy(3, fb, fp)
    other.start()
    other.wait_recv()
    pair = jnp.concatenate([f, fp[...]], axis=0)
    fh, fl = split(pair)
    th, tl = split(jnp.where(core == 0, pair[:, :COLS // 2], pair[:, COLS // 2:]).T)
    product = dot3(th, tl, fh, fl)
    for j in range(NODES):
        ga[j] = product[j * PIECE:(j + 1) * PIECE]
    gr[n] = ga[n]
    finish, sent_g = spread("node", NODES, n, ga, gr, gss, grs, True)
    finish()
    total = gr[0]
    for j in range(1, NODES):
        total = total + gr[j]
    pa[...] = total
    pr[z] = total

    def column(d):
        level = lax.rem(z + d, HEIGHT)
        return pltpu.make_async_remote_copy(
            src_ref=pa, dst_ref=pr.at[z], send_sem=hss.at[d], recv_sem=hrs.at[z],
            device_id={"row": 2 * level + core}, device_id_type=MESH)

    def column_arrival(d):
        level = lax.rem(z + d, HEIGHT)
        return pltpu.make_async_remote_copy(
            src_ref=pa, dst_ref=pr.at[level], send_sem=hss.at[d], recv_sem=hrs.at[level],
            device_id={"row": 2 * level + core}, device_id_type=MESH)

    @pl.loop(1, HEIGHT)
    def _(d):
        column(d).start()

    @pl.loop(1, HEIGHT)
    def _(d):
        column_arrival(d).wait_recv()

    total = pr[0]
    for j in range(1, HEIGHT):
        total = total + pr[j]
    total = total * (NODES / (ROWS * BS))
    qa[...] = total
    go[core, n] = total

    def result(side, d):
        return pltpu.make_async_remote_copy(
            src_ref=qa, dst_ref=go.at[core, n], send_sem=qss.at[side, d], recv_sem=qrs.at[core, n],
            device_id={"node": lax.rem(n + d, NODES), "row": partner if side else k}, device_id_type=MESH)

    def result_arrival(side, d):
        peer = lax.rem(n + d, NODES)
        source = 1 - core if side else core
        return pltpu.make_async_remote_copy(
            src_ref=qa, dst_ref=go.at[source, peer], send_sem=qss.at[side, d], recv_sem=qrs.at[source, peer],
            device_id={"node": peer, "row": partner if side else k}, device_id_type=MESH)

    def results(step):
        @pl.loop(1, NODES)
        def _(d):
            step(0, d)
            step(1, d)

        step(1, 0)

    results(lambda side, d: result(side, d).start())
    results(lambda side, d: result_arrival(side, d).wait_recv())
    for c in range(2):
        for j in range(NODES):
            at = c * (COLS // 2) + j * PIECE
            gram[at:at + PIECE, :] = go[c, j]

    probe.wait_send()

    @pl.when((core == 1) | ((z > 0) & (z < top)))
    def _():
        @pl.loop(0, PARTS)
        def _(b):
            operator(b).wait_send()

    @pl.when(core == 0)
    def _():
        second.wait_send()

        @chunks
        def _(q):
            inner(q).wait_send()
            term(q).wait_send()

    @pl.when(core == 1)
    def _():
        @chunks
        def _(q):
            solved(q).wait_send()

        @pl.when(z > 0)
        def _():
            @chunks
            def _(q):
                relay(q).wait_send()
                backward(q).wait_send()

        @pl.when(z < top)
        def _():
            @chunks
            def _(q):
                forward(q).wait_send()
                upper(q).wait_send()

    sent_x()
    sent_g()
    other.wait_send()

    @pl.loop(1, HEIGHT)
    def _(d):
        column(d).wait_send()

    results(lambda side, d: result(side, d).wait_send())


def shards(inv_factors, coupling, vectors):
    chunk = pltpu.VMEM((NCH, CH, BS), F32)
    whole = pltpu.VMEM((BS, 2 * BS), F32)
    whole_part = pltpu.VMEM((BS, 2 * BS), BF16)
    square_part = pltpu.VMEM((BS, BS), BF16)
    moments, gram = pl.pallas_call(
        kernel,
        out_shape=(
            jax.ShapeDtypeStruct((SHARE, COLS), F32),
            jax.ShapeDtypeStruct((COLS, COLS), F32),
        ),
        in_specs=[pl.BlockSpec(memory_space=pltpu.VMEM)] * 3,
        out_specs=[pl.BlockSpec(memory_space=pltpu.VMEM)] * 2,
        scratch_shapes=[
            pltpu.VMEM((NCH, HALF, BS), F32),
        ]
        + [whole_part] * 2
        + [square_part] * 4
        + [whole_part] * 8
        + [whole] * 3
        + [chunk] * 13
        + [
            pltpu.VMEM((2 * NVEC, BS), F32),
            pltpu.VMEM((NODES, SHARE, 2 * NVEC), F32),
            pltpu.VMEM((NODES, SHARE, 2 * NVEC), F32),
            pltpu.VMEM((NODES, PIECE, COLS), F32),
            pltpu.VMEM((NODES, PIECE, COLS), F32),
            pltpu.VMEM((PIECE, COLS), F32),
            pltpu.VMEM((HEIGHT, PIECE, COLS), F32),
            pltpu.VMEM((PIECE, COLS), F32),
            pltpu.VMEM((2, NODES, PIECE, COLS), F32),
            pltpu.VMEM((SHARE, COLS), F32),
            pltpu.VMEM((SHARE, COLS), F32),
        ]
        + [pltpu.SemaphoreType.DMA((PARTS,))] * 2
        + [pltpu.SemaphoreType.DMA((4,))] * 2
        + [pltpu.SemaphoreType.DMA((7, NCH))] * 2
        + [pltpu.SemaphoreType.DMA((16,))] * 6
        + [pltpu.SemaphoreType.DMA((2, 16))] * 2
        + [pltpu.SemaphoreType.REGULAR],
        compiler_params=pltpu.CompilerParams(
            collective_id=0, has_side_effects=True, vmem_limit_bytes=40 * 1024 * 1024),
    )(inv_factors, coupling, jnp.swapaxes(vectors, 1, 2).reshape(NCH, HALF, BS))
    return moments[None], gram


def solution(mesh):
    return jax.shard_map(
        shards,
        mesh=mesh,
        in_specs=(
            P(("intv", "node"), "row", None, None, None),
            P("row", None, None),
            P("row", None, None),
        ),
        out_specs=(P(("intv", "row"), "node", None), P("intv", None)),
        check_vma=False,
    )
```

```python
import math

import jax
import jax.numpy as jnp
from jax import lax
from jax.experimental import pallas as pl
from jax.experimental.pallas import tpu as pltpu
from jax.sharding import PartitionSpec as P

F32 = jnp.float32
BF16 = jnp.bfloat16
MESH = pl.DeviceIdType.MESH

BS = 512
NVEC = 64
NODES = 16
ROWS = 16
SHARE = BS // NODES
COLS = 256
PIECE = COLS // NODES // 2
NCH = 8
PARTS = 4
SIDE = 4
HEIGHT = ROWS // 2
HALF = NVEC // NCH
CH = 2 * HALF


def split(x):
    high = x.astype(BF16)
    return high, (x - high.astype(F32)).astype(BF16)


def dot(a, b):
    return jnp.dot(a, b, preferred_element_type=F32)


def dot3(ah, al, bh, bl):
    return dot(ah, bh) + (dot(ah, bl) + dot(al, bh))


def stacked(x):
    high, low = split(x)
    return jnp.concatenate([high, low], axis=0)


def complex_apply(x, wh, wl, groups=1):
    n = x.shape[0]
    high, low = split(x)
    z = dot(jnp.concatenate([high, low], axis=0), wh[...])
    z = z[:n] + (z[n:] + dot(high, wl[...]))
    h = n // groups // 2
    out = []
    for g in range(groups):
        re = slice(2 * g * h, (2 * g + 1) * h)
        im = slice((2 * g + 1) * h, (2 * g + 2) * h)
        out.append(z[re, :BS] - z[im, BS:])
        out.append(z[re, BS:] + z[im, :BS])
    return jnp.concatenate(out, axis=0)


def apply_all(x, wh, wl):
    return complex_apply(x.reshape(NCH * CH, BS), wh, wl, NCH).reshape(NCH, CH, BS)


def kernel(inv, coup, vt, mom, gram,
           vo, ath, atl, ch, cl, cth, ctl, mth, mtl, nth, ntl, pth, ptl, qth, qtl,
           snd, rcv, qf, yb, dd, fr, cf, fo, fs, us, uo, es, eo, br, xe, xs,
           xt, xa, xr, ga, gr, pa, pr, qa, go, fb, fp,
           oss, ors, pss, prs, css, crs, xss, xrs, gss, grs, hss, hrs, qss, qrs, plane_sem):
    k = lax.axis_index("row")
    n = lax.axis_index("node")
    core = lax.rem(k, 2)
    z = lax.div(k, 2)
    top = ROWS // 2 - 1
    partner = k + 1 - 2 * core

    barrier = pltpu.get_barrier_semaphore()

    def plane_signal(sem):
        across = lax.rem(n, SIDE)
        base = n - across
        for d in range(1, SIDE):
            pl.semaphore_signal(sem, inc=1, device_id={"node": base + lax.rem(across + d, SIDE)}, device_id_type=MESH)
            pl.semaphore_signal(sem, inc=1, device_id={"node": lax.rem(n + d * SIDE, NODES)}, device_id_type=MESH)

    plane_signal(barrier)

    pl.semaphore_signal(barrier, inc=1, device_id={"row": partner}, device_id_type=MESH)

    @pl.when(z > 0)
    def _():
        pl.semaphore_signal(barrier, inc=1, device_id={"row": k - 2}, device_id_type=MESH)

    @pl.when(z < top)
    def _():
        pl.semaphore_signal(barrier, inc=1, device_id={"row": k + 2}, device_id_type=MESH)

    for part in range(2):
        for b in range(4):
            high, low = split(inv[0, 0, part, b * 128:(b + 1) * 128, :].T)
            at = part * BS + b * 128
            ath[:, at:at + 128] = high
            atl[:, at:at + 128] = low
    for b in range(4):
        rows = slice(b * 128, (b + 1) * 128)
        block = coup[0, rows, :]
        high, low = split(block)
        ch[rows, :] = high
        cl[rows, :] = low

    def block_loop(count):
        def wrap(step):
            @pl.loop(0, count)
            def _(b):
                step(b, pl.ds(pl.multiple_of(b * (BS // count), BS // count), BS // count))
        return wrap

    def forward_operator(keep):
        @block_loop(4)
        def _(b, rows):
            for part in range(2):
                cols = slice(part * BS, (part + 1) * BS)
                value = dot3(ath[rows, cols], atl[rows, cols], ch[...], cl[...])
                if keep:
                    snd[rows, cols] = value
                high, low = split(value)
                mth[rows, cols] = high
                mtl[rows, cols] = low
            if keep:
                @pl.when(b == 0)
                def _():
                    enter()
                    probe.start()

                @pl.when((z > 0) & (z < top))
                def _():
                    operator(b).start()

    def backward_operator(keep):
        for b in range(4):
            rows = slice(b * 128, (b + 1) * 128)
            high, low = split(coup[0, rows, :].T)
            cth[:, rows] = high
            ctl[:, rows] = low

        @block_loop(4)
        def _(b, rows):
            for part in range(2):
                cols = slice(part * BS, (part + 1) * BS)
                value = dot3(cth[rows, :], ctl[rows, :], ath[:, cols], atl[:, cols])
                if keep:
                    snd[rows, cols] = value
                high, low = split(value)
                nth[rows, cols] = high
                ntl[rows, cols] = low
            if keep:
                operator(b).start()

    def compose(left, rows, wh, wl):
        x = jnp.concatenate([left[rows, :BS], left[rows, BS:]], axis=0)
        high, low = split(x)
        y = dot3(high, low, wh[...], wl[...])
        half = y.shape[0] // 2
        return y[:half, :BS] - y[half:, BS:], y[:half, BS:] + y[half:, :BS]

    def store_split(rows, parts, wh, wl):
        for part, value in enumerate(parts):
            cols = slice(part * BS, (part + 1) * BS)
            high, low = split(value)
            wh[rows, cols] = high
            wl[rows, cols] = low

    def chunk_copy(kind, source, target, row):
        def make(q):
            return pltpu.make_async_remote_copy(
                src_ref=source.at[q], dst_ref=target.at[q], send_sem=css.at[kind, q], recv_sem=crs.at[kind, q],
                device_id={"row": row}, device_id_type=MESH)
        return make

    def whole_copy(kind, source, target):
        return pltpu.make_async_remote_copy(
            src_ref=source, dst_ref=target, send_sem=pss.at[kind], recv_sem=prs.at[kind],
            device_id={"row": partner}, device_id_type=MESH)

    forward = chunk_copy(0, fs, fr, k + 2)
    relay = chunk_copy(1, fr, cf, partner)
    inner = chunk_copy(2, fs, fo, partner)
    upper = chunk_copy(3, us, uo, partner)
    term = chunk_copy(4, es, eo, partner)
    backward = chunk_copy(5, xe, br, k - 2)
    solved = chunk_copy(6, xe, xs, partner)

    def operator(b):
        rows = pl.ds(pl.multiple_of(b * (BS // PARTS), BS // PARTS), BS // PARTS)
        return pltpu.make_async_remote_copy(
            src_ref=snd.at[rows, :], dst_ref=rcv.at[rows, :], send_sem=oss.at[b], recv_sem=ors.at[b],
            device_id={"row": partner}, device_id_type=MESH)

    probe = whole_copy(1, vt, vo)
    second = whole_copy(2, qf, qf)

    def chunks(step):
        @pl.loop(0, NCH)
        def _(q):
            step(q)

    def shifted_by(carry, v):
        return jnp.concatenate([carry[:HALF] + v, carry[HALF:]], axis=0)

    def enter():
        ends = (z == 0).astype(jnp.int32) + (z == top).astype(jnp.int32)
        pl.semaphore_wait(barrier, 2 * (SIDE - 1) + 3 - ends)
        plane_signal(plane_sem)

    def real_rows(v):
        return jnp.concatenate([v, jnp.zeros_like(v)], axis=0)

    def even_forward(first):
        @chunks
        def _(q):
            if first:
                y = real_rows(vt[q])
            else:
                relay(q).wait_recv()
                y = shifted_by(cf[q], vt[q])
            yb[q] = y
            fs[q] = complex_apply(y, mth, mtl)
            inner(q).start()

    @pl.when(core == 0)
    def _():
        forward_operator(True)

        @pl.when(z == 0)
        def _():
            even_forward(True)

        backward_operator(False)
        probe.wait_recv()

        @pl.when(z < top)
        def _():
            @block_loop(PARTS)
            def _(b, rows):
                operator(b).wait_recv()
                re, im = compose(rcv, rows, nth, ntl)
                qf[rows, :BS] = re
                qf[rows, BS:] = im

        @pl.when(z == top)
        def _():
            @block_loop(PARTS)
            def _(b, rows):
                operator(b).wait_recv()
                store_split(rows, compose(rcv, rows, nth, ntl), pth, ptl)

            @block_loop(PARTS)
            def _(b, rows):
                re, im = compose(snd, rows, pth, ptl)
                qf[rows, :BS] = re + (ath[rows, :BS].astype(F32) + atl[rows, :BS].astype(F32))
                qf[rows, BS:] = im + (ath[rows, BS:].astype(F32) + atl[rows, BS:].astype(F32))

        second.start()

        @pl.when(z == top)
        def _():
            @chunks
            def _(q):
                es[q] = complex_apply(real_rows(vo[q]), pth, ptl)
                term(q).start()

        @pl.when(z > 0)
        def _():
            even_forward(False)

        @pl.when(z < top)
        def _():
            us[...] = apply_all(yb[...], ath, atl)

            @chunks
            def _(q):
                upper(q).wait_recv()
                es[q] = us[q] + complex_apply(uo[q], nth, ntl)
                term(q).start()

        @chunks
        def _(q):
            solved(q).wait_recv()

    def odd_upper():
        @chunks
        def _(q):
            inner(q).wait_recv()
            us[q] = complex_apply(shifted_by(fo[q], vt[q]), ath, atl)
            upper(q).start()

    @pl.when(core == 1)
    def _():
        @pl.when(z == 0)
        def _():
            forward_operator(False)
            enter()
            probe.start()

            @chunks
            def _(q):
                inner(q).wait_recv()
                y = shifted_by(fo[q], vt[q])
                yb[q] = y
                fs[q] = complex_apply(y, mth, mtl)
                forward(q).start()

            us[...] = apply_all(yb[...], ath, atl)

            @chunks
            def _(q):
                upper(q).start()

            backward_operator(True)
            probe.wait_recv()

        @pl.when((z > 0) & (z < top))
        def _():
            forward_operator(False)
            enter()
            probe.start()
            dd[...] = apply_all(jnp.concatenate([vt[...], jnp.zeros_like(vt)], axis=1), mth, mtl)

            @block_loop(PARTS)
            def _(b, rows):
                operator(b).wait_recv()
                store_split(rows, compose(rcv, rows, mth, mtl), pth, ptl)

            probe.wait_recv()

            @pl.when(z > 1)
            def _():
                backward_operator(True)

            @chunks
            def _(q):
                forward(q).wait_recv()
                relay(q).start()
                fs[q] = dd[q] + complex_apply(shifted_by(fr[q], vo[q]), pth, ptl)
                forward(q).start()

            @pl.when(z == 1)
            def _():
                backward_operator(True)

            odd_upper()

        def take_second(wh, wl):
            second.wait_recv()

            @block_loop(8)
            def _(b, rows):
                store_split(rows, (qf[rows, :BS], qf[rows, BS:]), wh, wl)

        @pl.when(z == top)
        def _():
            enter()
            probe.start()

            @block_loop(PARTS)
            def _(b, rows):
                snd[rows, :] = ath[rows, :].astype(F32) + atl[rows, :].astype(F32)
                operator(b).start()

            probe.wait_recv()
            take_second(pth, ptl)

            @chunks
            def _(q):
                forward(q).wait_recv()
                relay(q).start()
                term(q).wait_recv()
                xe[q] = eo[q] + complex_apply(shifted_by(fr[q], vo[q]), pth, ptl)
                backward(q).start()
                solved(q).start()

            @chunks
            def _(q):
                inner(q).wait_recv()
                yb[q] = shifted_by(fo[q], vt[q])

            xs[...] = apply_all(yb[...], ath, atl)

        @pl.when(z < top)
        def _():
            take_second(qth, qtl)

            @chunks
            def _(q):
                term(q).wait_recv()
                backward(q).wait_recv()
                xe[q] = eo[q] + complex_apply(br[q], qth, qtl)

                @pl.when(z > 0)
                def _():
                    backward(q).start()

                solved(q).start()

            xs[...] = us[...] + apply_all(br[...], nth, ntl)

    pl.semaphore_wait(plane_sem, 2 * (SIDE - 1))

    for q in range(NCH):
        x = xs[q]
        xt[q * HALF:(q + 1) * HALF, :] = x[:HALF]
        xt[NVEC + q * HALF:NVEC + (q + 1) * HALF, :] = x[HALF:]
    for b in range(4):
        x = xt[:, b * 128:(b + 1) * 128].T
        for s in range(128 // SHARE):
            xa[b * (128 // SHARE) + s] = x[s * SHARE:(s + 1) * SHARE]
    xr[n] = xa[n]

    def spread(axis, count, me, source, target, send, recv, by_target):
        def copy(d):
            peer = lax.rem(me + d, count)
            return pltpu.make_async_remote_copy(
                src_ref=source.at[peer] if by_target else source, dst_ref=target.at[me],
                send_sem=send.at[d], recv_sem=recv.at[me],
                device_id={axis: peer}, device_id_type=MESH)

        def arrival(d):
            peer = lax.rem(me + d, count)
            return pltpu.make_async_remote_copy(
                src_ref=source.at[peer] if by_target else source, dst_ref=target.at[peer],
                send_sem=send.at[d], recv_sem=recv.at[peer],
                device_id={axis: peer}, device_id_type=MESH)

        @pl.loop(1, count)
        def _(d):
            copy(d).start()

        def finish():
            @pl.loop(1, count)
            def _(d):
                arrival(d).wait_recv()

        def sent():
            @pl.loop(1, count)
            def _(d):
                copy(d).wait_send()

        return finish, sent

    finish, sent_x = spread("node", NODES, n, xa, xr, xss, xrs, True)
    finish()

    parts = []
    lane = lax.broadcasted_iota(jnp.int32, (SHARE, 2 * NVEC), 1)
    for order in (1, 2):
        even = jnp.zeros((SHARE, 2 * NVEC), F32)
        odd = jnp.zeros((SHARE, 2 * NVEC), F32)
        for j in range(NODES):
            theta = 2.0 * math.pi * (j + 0.5) / NODES
            x = xr[j]
            even = even + (math.cos(order * theta) / NODES) * x
            odd = odd + (math.sin(order * theta) / NODES) * x
        odd = pltpu.roll(odd, NVEC, 1)
        parts.append(even + jnp.where(lane < NVEC, -odd, odd))
    f = jnp.concatenate(parts, axis=1)
    mom[...] = f

    fb[...] = f
    other = whole_copy(3, fb, fp)
    other.start()
    other.wait_recv()
    pair = jnp.concatenate([f, fp[...]], axis=0)
    fh, fl = split(pair)
    th, tl = split(jnp.where(core == 0, pair[:, :COLS // 2], pair[:, COLS // 2:]).T)
    product = dot3(th, tl, fh, fl)
    for j in range(NODES):
        ga[j] = product[j * PIECE:(j + 1) * PIECE]
    gr[n] = ga[n]
    finish, sent_g = spread("node", NODES, n, ga, gr, gss, grs, True)
    finish()
    total = gr[0]
    for j in range(1, NODES):
        total = total + gr[j]
    pa[...] = total
    pr[z] = total

    def column(d):
        level = lax.rem(z + d, HEIGHT)
        return pltpu.make_async_remote_copy(
            src_ref=pa, dst_ref=pr.at[z], send_sem=hss.at[d], recv_sem=hrs.at[z],
            device_id={"row": 2 * level + core}, device_id_type=MESH)

    def column_arrival(d):
        level = lax.rem(z + d, HEIGHT)
        return pltpu.make_async_remote_copy(
            src_ref=pa, dst_ref=pr.at[level], send_sem=hss.at[d], recv_sem=hrs.at[level],
            device_id={"row": 2 * level + core}, device_id_type=MESH)

    @pl.loop(1, HEIGHT)
    def _(d):
        column(d).start()

    @pl.loop(1, HEIGHT)
    def _(d):
        column_arrival(d).wait_recv()

    total = pr[0]
    for j in range(1, HEIGHT):
        total = total + pr[j]
    total = total * (NODES / (ROWS * BS))
    qa[...] = total
    go[core, n] = total

    def result(side, d):
        return pltpu.make_async_remote_copy(
            src_ref=qa, dst_ref=go.at[core, n], send_sem=qss.at[side, d], recv_sem=qrs.at[core, n],
            device_id={"node": lax.rem(n + d, NODES), "row": partner if side else k}, device_id_type=MESH)

    def result_arrival(side, d):
        peer = lax.rem(n + d, NODES)
        source = 1 - core if side else core
        return pltpu.make_async_remote_copy(
            src_ref=qa, dst_ref=go.at[source, peer], send_sem=qss.at[side, d], recv_sem=qrs.at[source, peer],
            device_id={"node": peer, "row": partner if side else k}, device_id_type=MESH)

    def results(step):
        @pl.loop(1, NODES)
        def _(d):
            step(0, d)
            step(1, d)

        step(1, 0)

    results(lambda side, d: result(side, d).start())
    results(lambda side, d: result_arrival(side, d).wait_recv())
    for c in range(2):
        for j in range(NODES):
            at = c * (COLS // 2) + j * PIECE
            gram[at:at + PIECE, :] = go[c, j]

    probe.wait_send()

    @pl.when((core == 1) | ((z > 0) & (z < top)))
    def _():
        @pl.loop(0, PARTS)
        def _(b):
            operator(b).wait_send()

    @pl.when(core == 0)
    def _():
        second.wait_send()

        @chunks
        def _(q):
            inner(q).wait_send()
            term(q).wait_send()

    @pl.when(core == 1)
    def _():
        @chunks
        def _(q):
            solved(q).wait_send()

        @pl.when(z > 0)
        def _():
            @chunks
            def _(q):
                relay(q).wait_send()
                backward(q).wait_send()

        @pl.when(z < top)
        def _():
            @chunks
            def _(q):
                forward(q).wait_send()
                upper(q).wait_send()

    sent_x()
    sent_g()
    other.wait_send()

    @pl.loop(1, HEIGHT)
    def _(d):
        column(d).wait_send()

    results(lambda side, d: result(side, d).wait_send())


def shards(inv_factors, coupling, vectors):
    chunk = pltpu.VMEM((NCH, CH, BS), F32)
    whole = pltpu.VMEM((BS, 2 * BS), F32)
    whole_part = pltpu.VMEM((BS, 2 * BS), BF16)
    square_part = pltpu.VMEM((BS, BS), BF16)
    moments, gram = pl.pallas_call(
        kernel,
        out_shape=(
            jax.ShapeDtypeStruct((SHARE, COLS), F32),
            jax.ShapeDtypeStruct((COLS, COLS), F32),
        ),
        in_specs=[pl.BlockSpec(memory_space=pltpu.VMEM)] * 3,
        out_specs=[pl.BlockSpec(memory_space=pltpu.VMEM)] * 2,
        scratch_shapes=[
            pltpu.VMEM((NCH, HALF, BS), F32),
        ]
        + [whole_part] * 2
        + [square_part] * 4
        + [whole_part] * 8
        + [whole] * 3
        + [chunk] * 13
        + [
            pltpu.VMEM((2 * NVEC, BS), F32),
            pltpu.VMEM((NODES, SHARE, 2 * NVEC), F32),
            pltpu.VMEM((NODES, SHARE, 2 * NVEC), F32),
            pltpu.VMEM((NODES, PIECE, COLS), F32),
            pltpu.VMEM((NODES, PIECE, COLS), F32),
            pltpu.VMEM((PIECE, COLS), F32),
            pltpu.VMEM((HEIGHT, PIECE, COLS), F32),
            pltpu.VMEM((PIECE, COLS), F32),
            pltpu.VMEM((2, NODES, PIECE, COLS), F32),
            pltpu.VMEM((SHARE, COLS), F32),
            pltpu.VMEM((SHARE, COLS), F32),
        ]
        + [pltpu.SemaphoreType.DMA((PARTS,))] * 2
        + [pltpu.SemaphoreType.DMA((4,))] * 2
        + [pltpu.SemaphoreType.DMA((7, NCH))] * 2
        + [pltpu.SemaphoreType.DMA((16,))] * 6
        + [pltpu.SemaphoreType.DMA((2, 16))] * 2
        + [pltpu.SemaphoreType.REGULAR],
        compiler_params=pltpu.CompilerParams(
            collective_id=0, has_side_effects=True, vmem_limit_bytes=40 * 1024 * 1024),
    )(inv_factors, coupling, jnp.swapaxes(vectors, 1, 2).reshape(NCH, HALF, BS))
    return moments[None], gram


def solution(mesh):
    return jax.shard_map(
        shards,
        mesh=mesh,
        in_specs=(
            P(("intv", "node"), "row", None, None, None),
            P("row", None, None),
            P("row", None, None),
        ),
        out_specs=(P(("intv", "row"), "node", None), P("intv", None)),
        check_vma=False,
    )
```
